32 devices in a mesh: tm: 4 (over x, core), space: 8 (over z, y).
Axes of the slice: x: 2, y: 2, z: 4, core: 2. Of those that a mesh axis runs over, the one named last changes fastest.
Arguments:
- obs_perturb: bfloat16 [4, 32, 1024, 256], P('tm', 'space'), may hold values from -1.796875 to 1.796875
- innovation: float32 [4, 32, 1024], P('tm', 'space'), may hold values from -12 to 12
- error_weight: float32 [4, 32, 1024], P('tm', 'space'), may hold values from 0.5 to 2
- obs_column: int32 [4, 32, 1024], P('tm', 'space'), may hold values from 0 to 31
- obs_count: int32 [4, 32], P('tm', 'space'), may hold values from 64 to 1024, as said below
- radius: int32 [32], P('space'), may hold values from 56 to 80
- states: bfloat16 [8, 1024, 16, 256], P('tm', 'space'), may hold values from -6 to 6
Outputs:
- analysis: bfloat16 [8, 1024, 16, 256], P('tm', 'space')
The draws below stay inside these ranges and needn't reach their ends.
Inputs may be any that keep to these rules, and one draw needn't show every extreme that they name: `obs_count`: at most 1024; some slot and region holds exactly 1024 in every draw.
All inputs are finite; a program needn't handle non-finite values.
Results may differ from the reference program's by a relative error of at most 0.0065.
Values may be sent and summed in bfloat16 or wider, within the bound.
A program may use at most 64 MiB of HBM per device.

```python
import math
import jax
import jax.numpy as jnp
from jax import lax

K = 256
HC = 32
LEV = 16
OBS_CAP = 1024
NS_ITERS = 5
SLOTS = 4
LAGS = 8
REGIONS = 32
COLUMNS = 1024


def draw_obs_count(key, part):
    heavy_key, high_key, low_key, pick_key = jax.random.split(key, 4)
    grid_shape = (SLOTS, REGIONS)
    heavy_mask = jax.random.randint(heavy_key, grid_shape, 0, 4) == 0
    high_count = jax.random.randint(high_key, grid_shape, OBS_CAP // 2, OBS_CAP + 1)
    low_count = jax.random.randint(low_key, grid_shape, OBS_CAP // 16, OBS_CAP // 4 + 1)
    counts = jnp.where(heavy_mask, high_count, low_count).reshape(-1)
    chosen = jax.random.randint(pick_key, (), 0, SLOTS * REGIONS)
    counts = counts.at[chosen].set(OBS_CAP)
    return counts.reshape(grid_shape).astype(jnp.int32)


def place_ends(drawn, own_key, smallest, top_value):
    dims = drawn.shape
    place = [jax.random.randint(jax.random.fold_in(own_key, axis), (), 0, dims[axis]) for axis in range(len(dims))]
    drawn = drawn.at[tuple(place)].set(smallest)
    longest = dims.index(max(dims))
    place[longest] = (place[longest] + 1) % dims[longest]
    return drawn.at[tuple(place)].set(top_value)


def shard_levels(rng, dims, pieces, low, largest):
    level = 1.0
    for dim, blocks in pieces:
        draws = jax.random.uniform(jax.random.fold_in(jax.random.fold_in(rng, 6), dim), (blocks,), jnp.float32, low / len(pieces), largest / len(pieces))
        level = level * jnp.repeat(jnp.exp(draws), dims[dim] // blocks).reshape((-1,) + (1,) * (len(dims) - 1 - dim))
    return level


def centred(stream_key, extent, deviation, reach, pieces=(), held_as=jnp.bfloat16):
    gain = shard_levels(stream_key, extent, pieces, -0.22, 0.18) if pieces else 1.0
    entries = jax.random.normal(stream_key, extent, jnp.float32) * deviation * gain
    return jnp.minimum(jnp.maximum(entries, -reach), reach).astype(held_as)


def setup_inputs(seed: int = 0) -> dict:
    keys = jax.random.split(jax.random.key(seed), 8)
    return {
        "obs_perturb": centred(keys[0], (SLOTS, REGIONS, OBS_CAP, K), 0.3, 1.796875, ((0, 4), (1, 8))),
        "innovation": centred(keys[1], (SLOTS, REGIONS, OBS_CAP), 2.0, 12.0, ((0, 4), (1, 8)), jnp.float32),
        "error_weight": jnp.clip(jnp.exp(math.log(2.0) - 1.3862944 * jax.random.uniform(keys[2], (SLOTS, REGIONS, OBS_CAP), jnp.float32) ** shard_levels(keys[2], (SLOTS, REGIONS, OBS_CAP), ((0, 4), (1, 8)), -0.2, 0.2)), 0.5, 2.0),
        "obs_column": place_ends(jax.random.randint(keys[3], (SLOTS, REGIONS, OBS_CAP), 0, HC), jax.random.fold_in(keys[3], 1), 0, HC - 1).astype(jnp.int32),
        "obs_count": draw_obs_count(jax.random.fold_in(keys[7], 71), 0),
        "radius": place_ends(jax.random.randint(keys[5], (REGIONS,), 7 * HC // 4, 5 * HC // 2 + 1), jax.random.fold_in(keys[5], 1), 7 * HC // 4, (5 * HC // 2 + 1) - 1).astype(jnp.int32),
        "states": centred(keys[6], (LAGS, COLUMNS, LEV, K), 1.0, 6.0, ((0, 4), (1, 8))),
    }


INFLATION = 1.1
HIGHEST = lax.Precision.HIGHEST

def taper(column, radius, offset, width):
    distance = jnp.abs(column.astype(jnp.float32) + 0.5 - 0.5 * width - offset * width)
    ratio = jnp.minimum(distance / radius.astype(jnp.float32), 1.0)
    return jnp.square(1.0 - ratio * ratio)

def ensemble_transform(gram_sum, innov_sum):
    members = gram_sum.shape[-1]
    identity = jnp.eye(members, dtype=jnp.float32)
    system = gram_sum + (members - 1) / INFLATION * identity
    frobenius = jnp.sqrt(lax.optimization_barrier(jnp.sum(system * system, axis=(1, 2))))
    root_now = system / frobenius[:, None, None]
    inverse = jnp.broadcast_to(identity, system.shape)
    for iteration in range(NS_ITERS):
        middle = 1.5 * identity - 0.5 * jnp.einsum('nij,njk->nik', inverse, root_now, precision=HIGHEST)
        root_now = jnp.einsum('nij,njk->nik', root_now, middle, precision=HIGHEST)
        inverse = jnp.einsum('nij,njk->nik', middle, inverse, precision=HIGHEST)
    spread_part = jnp.sqrt(members - 1.0) * inverse / jnp.sqrt(frobenius)[:, None, None]
    half_step = jnp.einsum('nij,nj->ni', inverse, innov_sum, precision=HIGHEST)
    mean_part = jnp.einsum('nij,nj->ni', inverse, half_step, precision=HIGHEST) / frobenius[:, None]
    return spread_part + mean_part[:, :, None]

def reference(obs_perturb, innovation, error_weight, obs_column, obs_count, radius, states):
    slot_count, region_count, capacity, members = obs_perturb.shape
    position = lax.broadcasted_iota(jnp.int32, (slot_count, region_count, capacity), 2)
    present = (position < obs_count[:, :, None]).astype(jnp.float32)
    base_weight = error_weight * present
    weights = jnp.stack([base_weight * taper(obs_column, radius[None, :, None], offset, HC) for offset in range(-2, 3)])

    def region_gram(target):
        gram_sum = jnp.zeros((members, members), jnp.float32)
        vec_sum = jnp.zeros((members,), jnp.float32)
        for term_index, offset in enumerate(range(-2, 3)):
            source = (target - offset) % region_count
            source_rows = obs_perturb[:, source].reshape(-1, members)
            weight = weights[term_index][:, source].reshape(-1)
            weighted = (source_rows * weight[:, None]).astype(jnp.bfloat16)
            gram_sum = gram_sum + jnp.dot(weighted.T, source_rows, preferred_element_type=jnp.float32)
            vec_sum = vec_sum + jnp.dot(weighted.astype(jnp.float32).T, innovation[:, source].reshape(-1), precision=HIGHEST)
        return (gram_sum, vec_sum)
    gram_all, vec_all = lax.map(region_gram, jnp.arange(region_count, dtype=jnp.int32))
    transform = ensemble_transform(gram_all, vec_all).astype(jnp.bfloat16)
    preceding = jnp.roll(transform, 1, axis=0)
    following = jnp.roll(transform, -1, axis=0)
    lag_count = states.shape[0]
    levels = states.shape[2]
    shaped = states.reshape(lag_count, region_count, HC, levels, members)
    half_width = HC // 2
    blend_weight = jnp.abs((jnp.arange(HC, dtype=jnp.float32) + 0.5) / HC - 0.5).reshape(1, HC, 1, 1)

    def region_update(target):
        region_state = shaped[:, target]
        mean_state = lax.optimization_barrier(jnp.mean(region_state.astype(jnp.float32), axis=-1, keepdims=True))
        anomaly = (region_state - mean_state).astype(jnp.bfloat16)
        centre = jnp.dot(anomaly.reshape(-1, members), transform[target], preferred_element_type=jnp.float32)
        centre = centre.reshape(lag_count, HC, levels, members)
        western = jnp.dot(anomaly[:, :half_width].reshape(-1, members), preceding[target], preferred_element_type=jnp.float32)
        eastern = jnp.dot(anomaly[:, half_width:].reshape(-1, members), following[target], preferred_element_type=jnp.float32)
        beside = jnp.concatenate([western.reshape(lag_count, half_width, levels, members), eastern.reshape(lag_count, HC - half_width, levels, members)], axis=1)
        return (mean_state + (1.0 - blend_weight) * centre + blend_weight * beside).astype(jnp.bfloat16)
    updated = lax.map(region_update, jnp.arange(region_count, dtype=jnp.int32))
    return jnp.moveaxis(updated, 0, 1).reshape(states.shape)
```

```python
import functools

import jax
import jax.numpy as jnp
from jax import lax
from jax.experimental import pallas as pl
from jax.experimental.pallas import tpu as pltpu
from jax.sharding import PartitionSpec as P

HC = 32
NS_ITERS = 5
INFLATION = 1.1
HALO = 2
REACH = 2 * HALO + 1
EXTRA = 16
MESH = pl.DeviceIdType.MESH
F32 = jnp.float32
BF16 = jnp.bfloat16


def iota2(shape, dim):
    return lax.broadcasted_iota(jnp.int32, shape, dim)


def pack(matrix, row):
    half = matrix.shape[0] // 2
    a, b, c = matrix[:half, :half], matrix[:half, half:], matrix[half:, half:]
    i, j = iota2((half, half), 0), iota2((half, half), 1)
    top = jnp.concatenate([b, jnp.where(j >= i, a, c)], axis=1)
    diagonal = jnp.sum(jnp.where(i == j, c, 0.0), axis=0, keepdims=True)
    second = jnp.concatenate([diagonal, jnp.zeros_like(diagonal)], axis=1)
    place = iota2((EXTRA, 2 * half), 0)
    extra = jnp.where(place == 0, row, jnp.where(place == 1, second, 0.0))
    return top, extra


def unpack(block):
    half = block.shape[0] - EXTRA
    b, d = block[:half, :half], block[:half, half:]
    row = block[half : half + 1]
    diagonal = block[half + 1 : half + 2, :half]
    i, j = iota2((half, half), 0), iota2((half, half), 1)
    flipped = d.T
    a = jnp.where(j >= i, d, flipped)
    c = jnp.where(i > j, d, jnp.where(i < j, flipped, diagonal))
    matrix = jnp.concatenate(
        [jnp.concatenate([a, b], axis=1), jnp.concatenate([b.T, c], axis=1)], axis=0
    )
    return matrix, row


def split(x):
    high = x.astype(BF16)
    return high, (x - high.astype(F32)).astype(BF16)


def dot3(x, m_high, m_low):
    x_high, x_low = split(x)
    dot = functools.partial(jnp.dot, preferred_element_type=F32)
    return dot(x_high, m_high) + (dot(x_high, m_low) + dot(x_low, m_high))


def transform_parts(gram, vec):
    members = gram.shape[0]
    identity = (iota2(gram.shape, 0) == iota2(gram.shape, 1)).astype(F32)
    system = gram + (members - 1) / INFLATION * identity
    frob = jnp.sqrt(jnp.sum(jnp.sum(system * system, axis=0, keepdims=True), axis=1, keepdims=True))
    product = system * (1.0 / frob)
    inverse = None
    for step in range(NS_ITERS):
        middle = 1.5 * identity - 0.5 * product
        m = split(middle)
        last = step == NS_ITERS - 1
        if inverse is None:
            inverse = middle
            moved = dot3(product, *m)
        elif last:
            inverse = dot3(inverse, *m)
        else:
            both = dot3(jnp.concatenate([product, inverse], axis=0), *m)
            moved, inverse = both[:members], both[members:]
        if not last:
            product = dot3(moved, *m)
    m = split(inverse)
    rows = jnp.broadcast_to(vec, (8, members))
    wbar = dot3(dot3(rows, *m), *m)[0:1] / frob
    spread = inverse * (jnp.sqrt(F32(members - 1.0)) / jnp.sqrt(frob))
    return spread, wbar


def assimilate(
    n_tm, n_space,
    count_ref, radius_ref, obs_hbm, innov_ref, weight_ref, column_ref, out_ref,
    obs_v, obs_t, mine, recv, halo_out, halo_in, t_out, t_in,
    load_sem, rs_send, rs_recv, halo_send, halo_recv, t_send, b_send, t_recv,
):
    tm, sp = lax.axis_index("tm"), lax.axis_index("space")
    after, before = lax.rem(sp + 1, n_space), lax.rem(sp + n_space - 1, n_space)
    regions, capacity, members = obs_v.shape
    half = members // 2
    targets = regions + 2 * HALO

    loads = [
        pltpu.make_async_copy(obs_hbm.at[0, r], obs_v.at[r], load_sem.at[r]) for r in range(regions)
    ]
    for load in loads:
        load.start()

    barrier = pltpu.get_barrier_semaphore()
    peers = [lax.rem(tm + d, n_tm) for d in range(1, n_tm)]
    greeted = [(p, sp) for p in peers]
    greeted += [(t, s) for s in (before, after) for t in range(n_tm)]
    for t, s in greeted:
        pl.semaphore_signal(barrier, inc=1, device_id={"tm": t, "space": s}, device_id_type=MESH)

    shape = (regions, capacity)
    which = iota2(shape, 0)
    count = jnp.zeros(shape, jnp.int32)
    radius = jnp.zeros(shape, jnp.int32)
    for r in range(regions):
        count = jnp.where(which == r, count_ref[0, r], count)
        radius = jnp.where(which == r, radius_ref[r], radius)
    present = (iota2(shape, 1) < count).astype(F32)
    base = weight_ref[0] * present
    inverse_radius = 1.0 / radius.astype(F32)
    position = column_ref[0].astype(F32) + 0.5 - 0.5 * HC
    weights, pulls = [], []
    for offset in range(-HALO, HALO + 1):
        ratio = jnp.minimum(jnp.abs(position - offset * HC) * inverse_radius, 1.0)
        weight = base * jnp.square(1.0 - ratio * ratio)
        weights.append(weight)
        pulls.append(weight * innov_ref[0])

    first_row = iota2((EXTRA, capacity), 0) == 0

    def gram_of(target):
        total = None
        for r in range(max(0, target - 2 * HALO), min(regions, target + 1)):
            k = target - r
            weight = jnp.broadcast_to(weights[k][r : r + 1], (16, capacity)).astype(BF16)
            pull = jnp.where(first_row, pulls[k][r : r + 1], 0.0).astype(BF16)
            scaled = obs_t[r].reshape(members // 16, 16, capacity) * weight[None]
            left = jnp.concatenate([scaled.reshape(members, capacity), pull], axis=0)
            part = jnp.dot(left, obs_v[r], preferred_element_type=F32)
            total = part if total is None else total + part
        top, extra = pack(total[:members], total[members : members + 1])
        mine[target, :half] = top.astype(BF16)
        mine[target, half:] = extra.astype(BF16)

    def exchange(kind, block_of):
        copies = []
        for d, peer in enumerate(peers):
            copies.append(
                pltpu.make_async_remote_copy(
                    src_ref=mine.at[block_of(peer)],
                    dst_ref=recv.at[kind, tm],
                    send_sem=rs_send.at[kind, d],
                    recv_sem=rs_recv.at[kind, tm],
                    device_id={"tm": peer, "space": sp},
                    device_id_type=MESH,
                )
            )
        return copies

    def collect(kind, block):
        total = mine[block].astype(F32)
        for peer in peers:
            pltpu.make_async_copy(
                recv.at[kind, peer], recv.at[kind, peer], rs_recv.at[kind, peer]
            ).wait()
            total = total + recv[kind, peer].astype(F32)
        return total

    for r in range(regions):
        loads[r].wait()
        obs_t[r] = obs_v[r].T
    pl_wait = len(greeted)
    edges = [*range(HALO), *range(targets - HALO, targets)]
    for target in edges:
        gram_of(target)
    pl.semaphore_wait(barrier, pl_wait)
    edge_block = lambda p: lax.rem(p + regions + HALO, targets)
    inner_block = lambda p: p + HALO
    edge_copies = exchange(0, edge_block)
    for copy in edge_copies:
        copy.start()
    inner = list(range(HALO, targets - HALO))
    for target in inner:
        gram_of(target)
    inner_copies = exchange(1, inner_block)
    for copy in inner_copies:
        copy.start()

    halo_out[...] = collect(0, edge_block(tm)).astype(BF16)
    halo_copy = pltpu.make_async_remote_copy(
        src_ref=halo_out,
        dst_ref=halo_in,
        send_sem=halo_send,
        recv_sem=halo_recv,
        device_id={"tm": tm, "space": jnp.where(tm < HALO, after, before)},
        device_id_type=MESH,
    )
    halo_copy.start()
    total = collect(1, inner_block(tm))
    halo_copy.wait()
    gram, vec = unpack(total + halo_in[...].astype(F32))
    spread, wbar = transform_parts(gram, vec)
    top, extra = pack(spread, wbar)
    t_out[:half] = top.astype(BF16)
    t_out[half:] = extra.astype(BF16)

    def send_transform(t, s, slot, sem):
        return pltpu.make_async_remote_copy(
            src_ref=t_out,
            dst_ref=t_in.at[slot],
            send_sem=sem,
            recv_sem=t_recv.at[slot],
            device_id={"tm": t, "space": s},
            device_id_type=MESH,
        )

    low = [send_transform(t, before, regions + 1, b_send.at[t]) for t in range(n_tm)]
    high = [send_transform(t, after, 0, b_send.at[t]) for t in range(n_tm)]

    @pl.when(tm == 0)
    def _():
        for copy in low:
            copy.start()

    @pl.when(tm == n_tm - 1)
    def _():
        for copy in high:
            copy.start()

    t_copies = [send_transform(p, sp, tm + 1, t_send.at[d]) for d, p in enumerate(peers)]
    for copy in t_copies:
        copy.start()

    def place(slot, block):
        matrix, row = unpack(block.astype(F32))
        out_ref[slot] = (matrix + row).astype(BF16)

    place(tm + 1, t_out[...])
    for slot in [lax.rem(tm + d, n_tm) + 1 for d in range(1, n_tm)] + [0, regions + 1]:
        pltpu.make_async_copy(t_in.at[slot], t_in.at[slot], t_recv.at[slot]).wait()
        place(slot, t_in[slot])

    for copy in edge_copies + inner_copies + t_copies:
        copy.wait_send()

    @pl.when(tm == 0)
    def _():
        for copy in low:
            copy.wait_send()

    @pl.when(tm == n_tm - 1)
    def _():
        for copy in high:
            copy.wait_send()


def analyse(transform_ref, states_ref, out_ref):
    region = pl.program_id(1)
    x = states_ref[0, 0].astype(F32)
    rows, members = x.shape
    mean = jnp.sum(x, axis=1, keepdims=True) * (1.0 / members)
    anomaly = (x - mean).astype(BF16)
    mid = rows // 2

    def apply(block, slot):
        return lax.dot_general(
            block, transform_ref[slot], (((1,), (1,)), ((), ())), preferred_element_type=F32
        )

    centre = apply(anomaly, region + 1)
    beside = jnp.concatenate(
        [apply(anomaly[:mid], region), apply(anomaly[mid:], region + 2)], axis=0
    )
    column = iota2((rows, 1), 0) // (rows // HC)
    blend = jnp.abs((column.astype(F32) + 0.5) / HC - 0.5)
    out_ref[0, 0] = (mean + centre + blend * (beside - centre)).astype(BF16)


def shards(n_tm, n_space, obs, innovation, error_weight, obs_column, obs_count, radius, states):
    _, regions, capacity, members = obs.shape
    assert regions == n_tm and obs.shape[0] == 1
    rows = members // 2 + EXTRA
    vmem = pl.BlockSpec(memory_space=pltpu.VMEM)
    smem = pl.BlockSpec(memory_space=pltpu.SMEM)
    hbm = pl.BlockSpec(memory_space=pl.ANY)
    dma = pltpu.SemaphoreType.DMA
    transforms = pl.pallas_call(
        functools.partial(assimilate, n_tm, n_space),
        out_shape=jax.ShapeDtypeStruct((regions + 2, members, members), BF16),
        in_specs=[smem, smem, hbm, vmem, vmem, vmem],
        out_specs=vmem,
        scratch_shapes=[
            pltpu.VMEM((regions, capacity, members), BF16),
            pltpu.VMEM((regions, members, capacity), BF16),
            pltpu.VMEM((regions + 2 * HALO, rows, members), BF16),
            pltpu.VMEM((2, n_tm, rows, members), BF16),
            pltpu.VMEM((rows, members), BF16),
            pltpu.VMEM((rows, members), BF16),
            pltpu.VMEM((rows, members), BF16),
            pltpu.VMEM((regions + 2, rows, members), BF16),
            dma((regions,)),
            dma((2, n_tm - 1)),
            dma((2, n_tm)),
            dma,
            dma,
            dma((n_tm - 1,)),
            dma((n_tm,)),
            dma((regions + 2,)),
        ],
        compiler_params=pltpu.CompilerParams(
            collective_id=0, has_side_effects=True, vmem_limit_bytes=40 * 2**20
        ),
        name="assimilate",
    )(obs_count, radius, obs, innovation, error_weight, obs_column)
    lags, columns, levels, _ = states.shape
    shaped = states.reshape(lags, regions, columns // regions * levels, members)
    block = pl.BlockSpec((1, 1) + shaped.shape[2:], lambda i, j: (i, j, 0, 0))
    result = pl.pallas_call(
        analyse,
        grid=(lags, regions),
        out_shape=jax.ShapeDtypeStruct(shaped.shape, BF16),
        in_specs=[vmem, block],
        out_specs=block,
        compiler_params=pltpu.CompilerParams(vmem_limit_bytes=20 * 2**20),
        name="analyse",
    )(transforms, shaped)
    return result.reshape(states.shape)


def solution(mesh):
    return jax.shard_map(
        functools.partial(shards, mesh.shape["tm"], mesh.shape["space"]),
        mesh=mesh,
        in_specs=(
            P("tm", "space", None, None),
            P("tm", "space", None),
            P("tm", "space", None),
            P("tm", "space", None),
            P("tm", "space"),
            P("space"),
            P("tm", "space", None, None),
        ),
        out_specs=P("tm", "space", None, None),
        check_vma=False,
    )
```

```python
import functools

import jax
import jax.numpy as jnp
from jax import lax
from jax.experimental import pallas as pl
from jax.experimental.pallas import tpu as pltpu
from jax.sharding import PartitionSpec as P

HC = 32
NS_ITERS = 5
INFLATION = 1.1
HALO = 2
REACH = 2 * HALO + 1
EXTRA = 16
MESH = pl.DeviceIdType.MESH
F32 = jnp.float32
BF16 = jnp.bfloat16


def iota2(shape, dim):
    return lax.broadcasted_iota(jnp.int32, shape, dim)


def pack(matrix, row):
    half = matrix.shape[0] // 2
    a, b, c = matrix[:half, :half], matrix[:half, half:], matrix[half:, half:]
    i, j = iota2((half, half), 0), iota2((half, half), 1)
    top = jnp.concatenate([b, jnp.where(j >= i, a, c)], axis=1)
    diagonal = jnp.sum(jnp.where(i == j, c, 0.0), axis=0, keepdims=True)
    second = jnp.concatenate([diagonal, jnp.zeros_like(diagonal)], axis=1)
    place = iota2((EXTRA, 2 * half), 0)
    extra = jnp.where(place == 0, row, jnp.where(place == 1, second, 0.0))
    return top, extra


def unpack(block):
    half = block.shape[0] - EXTRA
    b, d = block[:half, :half], block[:half, half:]
    row = block[half : half + 1]
    diagonal = block[half + 1 : half + 2, :half]
    i, j = iota2((half, half), 0), iota2((half, half), 1)
    flipped = d.T
    a = jnp.where(j >= i, d, flipped)
    c = jnp.where(i > j, d, jnp.where(i < j, flipped, diagonal))
    matrix = jnp.concatenate(
        [jnp.concatenate([a, b], axis=1), jnp.concatenate([b.T, c], axis=1)], axis=0
    )
    return matrix, row


def split(x):
    high = x.astype(BF16)
    return high, (x - high.astype(F32)).astype(BF16)


def dot3(x, m_high, m_low):
    x_high, x_low = split(x)
    dot = functools.partial(jnp.dot, preferred_element_type=F32)
    return dot(x_high, m_high) + (dot(x_high, m_low) + dot(x_low, m_high))


def transform_parts(gram, vec):
    members = gram.shape[0]
    identity = (iota2(gram.shape, 0) == iota2(gram.shape, 1)).astype(F32)
    system = gram + (members - 1) / INFLATION * identity
    frob = jnp.sqrt(jnp.sum(jnp.sum(system * system, axis=0, keepdims=True), axis=1, keepdims=True))
    product = system * (1.0 / frob)
    inverse = None
    for step in range(NS_ITERS):
        middle = 1.5 * identity - 0.5 * product
        m = split(middle)
        last = step == NS_ITERS - 1
        if inverse is None:
            inverse = middle
            moved = dot3(product, *m)
        elif last:
            inverse = dot3(inverse, *m)
        else:
            both = dot3(jnp.concatenate([product, inverse], axis=0), *m)
            moved, inverse = both[:members], both[members:]
        if not last:
            product = dot3(moved, *m)
    m = split(inverse)
    rows = jnp.broadcast_to(vec, (8, members))
    wbar = dot3(dot3(rows, *m), *m)[0:1] / frob
    spread = inverse * (jnp.sqrt(F32(members - 1.0)) / jnp.sqrt(frob))
    return spread, wbar


def assimilate(
    n_tm, n_space,
    count_hbm, radius_hbm, obs_hbm, innov_hbm, weight_hbm, column_hbm, states_hbm, out_ref,
    count_ref, radius_ref, innov_ref, weight_ref, column_ref, anomaly, means, tmat, obs_v, obs_t, mine, recv, halo_out, halo_in, t_out, t_in,
    load_sem, small_sem, rs_send, rs_recv, halo_send, halo_recv, t_send, b_send, t_recv,
):
    tm, sp = lax.axis_index("tm"), lax.axis_index("space")
    after, before = lax.rem(sp + 1, n_space), lax.rem(sp + n_space - 1, n_space)
    regions, capacity, members = obs_v.shape
    half = members // 2
    targets = regions + 2 * HALO

    loads = [
        pltpu.make_async_copy(obs_hbm.at[0, r], obs_v.at[r], load_sem.at[r]) for r in range(regions)
    ]
    small = [
        pltpu.make_async_copy(src, dst, small_sem.at[n])
        for n, (src, dst) in enumerate(
            [
                (count_hbm, count_ref),
                (radius_hbm, radius_ref),
                (innov_hbm.at[0], innov_ref),
                (weight_hbm.at[0], weight_ref),
                (column_hbm.at[0], column_ref),
                (states_hbm, anomaly),
            ]
        )
    ]
    for load in small[:-1] + loads + small[-1:]:
        load.start()

    barrier = pltpu.get_barrier_semaphore()
    peers = [lax.rem(tm + d, n_tm) for d in range(1, n_tm)]
    greeted = [(p, sp) for p in peers]
    greeted += [(t, s) for s in (before, after) for t in range(n_tm)]
    for t, s in greeted:
        pl.semaphore_signal(barrier, inc=1, device_id={"tm": t, "space": s}, device_id_type=MESH)

    for r in range(regions):
        loads[r].wait()
        obs_t[r] = obs_v[r].T
    for load in small[:-1]:
        load.wait()

    shape = (regions, capacity)
    which = iota2(shape, 0)
    count = jnp.zeros(shape, jnp.int32)
    radius = jnp.zeros(shape, jnp.int32)
    for r in range(regions):
        count = jnp.where(which == r, count_ref[0, r], count)
        radius = jnp.where(which == r, radius_ref[r], radius)
    present = (iota2(shape, 1) < count).astype(F32)
    base = weight_ref[...] * present
    inverse_radius = 1.0 / radius.astype(F32)
    position = column_ref[...].astype(F32) + 0.5 - 0.5 * HC
    weights, pulls = [], []
    for offset in range(-HALO, HALO + 1):
        ratio = jnp.minimum(jnp.abs(position - offset * HC) * inverse_radius, 1.0)
        weight = base * jnp.square(1.0 - ratio * ratio)
        weights.append(weight)
        pulls.append(weight * innov_ref[...])

    first_row = iota2((EXTRA, capacity), 0) == 0

    def gram_of(target):
        total = None
        for r in range(max(0, target - 2 * HALO), min(regions, target + 1)):
            k = target - r
            weight = jnp.broadcast_to(weights[k][r : r + 1], (16, capacity)).astype(BF16)
            pull = jnp.where(first_row, pulls[k][r : r + 1], 0.0).astype(BF16)
            scaled = obs_t[r].reshape(members // 16, 16, capacity) * weight[None]
            left = jnp.concatenate([scaled.reshape(members, capacity), pull], axis=0)
            part = jnp.dot(left, obs_v[r], preferred_element_type=F32)
            total = part if total is None else total + part
        top, extra = pack(total[:members], total[members : members + 1])
        mine[target, :half] = top.astype(BF16)
        mine[target, half:] = extra.astype(BF16)

    def exchange(kind, block_of):
        copies = []
        for d, peer in enumerate(peers):
            copies.append(
                pltpu.make_async_remote_copy(
                    src_ref=mine.at[block_of(peer)],
                    dst_ref=recv.at[kind, tm],
                    send_sem=rs_send.at[kind, d],
                    recv_sem=rs_recv.at[kind, tm],
                    device_id={"tm": peer, "space": sp},
                    device_id_type=MESH,
                )
            )
        return copies

    def collect(kind, block):
        total = mine[block].astype(F32)
        for peer in peers:
            pltpu.make_async_copy(
                recv.at[kind, peer], recv.at[kind, peer], rs_recv.at[kind, peer]
            ).wait()
            total = total + recv[kind, peer].astype(F32)
        return total

    edges = [*range(HALO), *range(targets - HALO, targets)]
    for target in edges:
        gram_of(target)
    pl.semaphore_wait(barrier, len(greeted))
    edge_block = lambda p: lax.rem(p + regions + HALO, targets)
    inner_block = lambda p: p + HALO
    edge_copies = exchange(0, edge_block)
    for copy in edge_copies:
        copy.start()
    inner = list(range(HALO, targets - HALO))
    for target in inner:
        gram_of(target)
    inner_copies = exchange(1, inner_block)
    for copy in inner_copies:
        copy.start()

    small[-1].wait()
    lags, _, rows, _ = anomaly.shape

    def centre_on_mean(n, carry):
        lag, r = n // regions, lax.rem(n, regions)
        x = anomaly[lag, r].astype(F32)
        mean = jnp.sum(x, axis=1, keepdims=True) * (1.0 / members)
        means[lag, r] = mean
        anomaly[lag, r] = (x - mean).astype(BF16)
        return carry

    lax.fori_loop(0, lags * regions, centre_on_mean, 0)

    halo_out[...] = collect(0, edge_block(tm)).astype(BF16)
    halo_copy = pltpu.make_async_remote_copy(
        src_ref=halo_out,
        dst_ref=halo_in,
        send_sem=halo_send,
        recv_sem=halo_recv,
        device_id={"tm": tm, "space": jnp.where(tm < HALO, after, before)},
        device_id_type=MESH,
    )
    halo_copy.start()
    total = collect(1, inner_block(tm))
    halo_copy.wait()
    gram, vec = unpack(total + halo_in[...].astype(F32))
    spread, wbar = transform_parts(gram, vec)
    top, extra = pack(spread, wbar)
    t_out[:half] = top.astype(BF16)
    t_out[half:] = extra.astype(BF16)

    def send_transform(t, s, slot, sem):
        return pltpu.make_async_remote_copy(
            src_ref=t_out,
            dst_ref=t_in.at[slot],
            send_sem=sem,
            recv_sem=t_recv.at[slot],
            device_id={"tm": t, "space": s},
            device_id_type=MESH,
        )

    low = [send_transform(t, before, regions + 1, b_send.at[t]) for t in range(n_tm)]
    high = [send_transform(t, after, 0, b_send.at[t]) for t in range(n_tm)]

    @pl.when(tm == 0)
    def _():
        for copy in low:
            copy.start()

    @pl.when(tm == n_tm - 1)
    def _():
        for copy in high:
            copy.start()

    t_copies = [send_transform(p, sp, tm + 1, t_send.at[d]) for d, p in enumerate(peers)]
    for copy in t_copies:
        copy.start()

    def place(slot, block):
        matrix, row = unpack(block.astype(F32))
        tmat[slot] = (matrix + row).astype(BF16)

    def arrive(slot):
        pltpu.make_async_copy(t_in.at[slot], t_in.at[slot], t_recv.at[slot]).wait()
        place(slot, t_in[slot])

    mid = rows // 2

    def update(r, side):
        part = slice(side * mid, (side + 1) * mid)
        column = (iota2((mid, 1), 0) + side * mid) // (rows // HC)
        blend = jnp.abs((column.astype(F32) + 0.5) / HC - 0.5)
        for lag in range(lags):
            block = anomaly[lag, r, part]

            def apply(slot):
                return lax.dot_general(
                    block, tmat[slot], (((1,), (1,)), ((), ())), preferred_element_type=F32
                )

            centre, beside = apply(r + 1), apply(r + 2 * side)
            mean = means[lag, r, part]
            out_ref[lag, r, part] = (mean + centre + blend * (beside - centre)).astype(BF16)

    place(tm + 1, t_out[...])
    for d in range(1, n_tm):
        arrive(lax.rem(tm + d, n_tm) + 1)
    for r in range(regions):
        for side in range(2):
            if (r, side) not in ((0, 0), (regions - 1, 1)):
                update(r, side)
    arrive(0)
    update(0, 0)
    arrive(regions + 1)
    update(regions - 1, 1)

    for copy in edge_copies + inner_copies + t_copies:
        copy.wait_send()

    @pl.when(tm == 0)
    def _():
        for copy in low:
            copy.wait_send()

    @pl.when(tm == n_tm - 1)
    def _():
        for copy in high:
            copy.wait_send()


def shards(n_tm, n_space, obs, innovation, error_weight, obs_column, obs_count, radius, states):
    _, regions, capacity, members = obs.shape
    assert regions == n_tm and obs.shape[0] == 1
    rows = members // 2 + EXTRA
    lags, columns, levels, _ = states.shape
    shaped = states.reshape(lags, regions, columns // regions * levels, members)
    hbm = pl.BlockSpec(memory_space=pltpu.HBM)
    dma = pltpu.SemaphoreType.DMA
    result = pl.pallas_call(
        functools.partial(assimilate, n_tm, n_space),
        out_shape=pltpu.VMEM(shaped.shape, BF16),
        in_specs=[hbm] * 7,
        out_specs=pl.BlockSpec(memory_space=pltpu.VMEM),
        scratch_shapes=[
            pltpu.SMEM(obs_count.shape, jnp.int32),
            pltpu.SMEM(radius.shape, jnp.int32),
            pltpu.VMEM((regions, capacity), F32),
            pltpu.VMEM((regions, capacity), F32),
            pltpu.VMEM((regions, capacity), jnp.int32),
            pltpu.VMEM(shaped.shape, BF16),
            pltpu.VMEM(shaped.shape[:-1] + (1,), F32),
            pltpu.VMEM((regions + 2, members, members), BF16),
            pltpu.VMEM((regions, capacity, members), BF16),
            pltpu.VMEM((regions, members, capacity), BF16),
            pltpu.VMEM((regions + 2 * HALO, rows, members), BF16),
            pltpu.VMEM((2, n_tm, rows, members), BF16),
            pltpu.VMEM((rows, members), BF16),
            pltpu.VMEM((rows, members), BF16),
            pltpu.VMEM((rows, members), BF16),
            pltpu.VMEM((regions + 2, rows, members), BF16),
            dma((regions,)),
            dma((6,)),
            dma((2, n_tm - 1)),
            dma((2, n_tm)),
            dma,
            dma,
            dma((n_tm - 1,)),
            dma((n_tm,)),
            dma((regions + 2,)),
        ],
        compiler_params=pltpu.CompilerParams(
            collective_id=0, has_side_effects=True, vmem_limit_bytes=67043328 - 2228224
        ),
        name="assimilate",
    )(obs_count, radius, obs, innovation, error_weight, obs_column, shaped)
    return result.reshape(states.shape)


def solution(mesh):
    return jax.shard_map(
        functools.partial(shards, mesh.shape["tm"], mesh.shape["space"]),
        mesh=mesh,
        in_specs=(
            P("tm", "space", None, None),
            P("tm", "space", None),
            P("tm", "space", None),
            P("tm", "space", None),
            P("tm", "space"),
            P("space"),
            P("tm", "space", None, None),
        ),
        out_specs=P("tm", "space", None, None),
        check_vma=False,
    )
```

```python
import functools

import jax
import jax.numpy as jnp
from jax import lax
from jax.experimental import pallas as pl
from jax.experimental.pallas import tpu as pltpu
from jax.sharding import PartitionSpec as P

HC = 32
NS_ITERS = 5
INFLATION = 1.1
HALO = 2
REACH = 2 * HALO + 1
EXTRA = 16
MESH = pl.DeviceIdType.MESH
F32 = jnp.float32
BF16 = jnp.bfloat16


def iota2(shape, dim):
    return lax.broadcasted_iota(jnp.int32, shape, dim)


def pack(matrix, row):
    half = matrix.shape[0] // 2
    a, b, c = matrix[:half, :half], matrix[:half, half:], matrix[half:, half:]
    i, j = iota2((half, half), 0), iota2((half, half), 1)
    top = jnp.concatenate([b, jnp.where(j >= i, a, c)], axis=1)
    diagonal = jnp.sum(jnp.where(i == j, c, 0.0), axis=0, keepdims=True)
    second = jnp.concatenate([diagonal, jnp.zeros_like(diagonal)], axis=1)
    place = iota2((EXTRA, 2 * half), 0)
    extra = jnp.where(place == 0, row, jnp.where(place == 1, second, 0.0))
    return top, extra


def unpack(block):
    half = block.shape[0] - EXTRA
    b, d = block[:half, :half], block[:half, half:]
    row = block[half : half + 1]
    diagonal = block[half + 1 : half + 2, :half]
    i, j = iota2((half, half), 0), iota2((half, half), 1)
    flipped = d.T
    a = jnp.where(j >= i, d, flipped)
    c = jnp.where(i > j, d, jnp.where(i < j, flipped, diagonal))
    matrix = jnp.concatenate(
        [jnp.concatenate([a, b], axis=1), jnp.concatenate([b.T, c], axis=1)], axis=0
    )
    return matrix, row


def split(x):
    high = x.astype(BF16)
    return high, (x - high.astype(F32)).astype(BF16)


def dot3(x, m_high, m_low):
    x_high, x_low = split(x)
    dot = functools.partial(jnp.dot, preferred_element_type=F32)
    return dot(x_high, m_high) + (dot(x_high, m_low) + dot(x_low, m_high))


def transform_parts(gram, vec):
    members = gram.shape[0]
    identity = (iota2(gram.shape, 0) == iota2(gram.shape, 1)).astype(F32)
    system = gram + (members - 1) / INFLATION * identity
    frob = jnp.sqrt(jnp.sum(jnp.sum(system * system, axis=0, keepdims=True), axis=1, keepdims=True))
    product = system * (1.0 / frob)
    inverse = None
    for step in range(NS_ITERS):
        middle = 1.5 * identity - 0.5 * product
        m = split(middle)
        last = step == NS_ITERS - 1
        if inverse is None:
            inverse = middle
            moved = dot3(product, *m)
        elif last:
            inverse = dot3(inverse, *m)
        else:
            both = dot3(jnp.concatenate([product, inverse], axis=0), *m)
            moved, inverse = both[:members], both[members:]
        if not last:
            product = dot3(moved, *m)
    m = split(inverse)
    rows = jnp.broadcast_to(vec, (8, members))
    wbar = dot3(dot3(rows, *m), *m)[0:1] / frob
    spread = inverse * (jnp.sqrt(F32(members - 1.0)) / jnp.sqrt(frob))
    return spread, wbar


def assimilate(
    n_tm, n_space,
    count_hbm, radius_hbm, obs_hbm, innov_hbm, weight_hbm, column_hbm, states_hbm, out_ref,
    count_ref, radius_ref, innov_ref, weight_ref, column_ref, anomaly, means, tmat, obs_v, obs_t, mine, recv, halo_out, halo_in, t_out, t_in,
    load_sem, small_sem, rs_send, rs_recv, halo_send, halo_recv, t_send, b_send, t_recv,
):
    tm, sp = lax.axis_index("tm"), lax.axis_index("space")
    after, before = lax.rem(sp + 1, n_space), lax.rem(sp + n_space - 1, n_space)
    regions, capacity, members = obs_v.shape
    half = members // 2
    targets = regions + 2 * HALO

    loads = [
        pltpu.make_async_copy(obs_hbm.at[0, r], obs_v.at[r], load_sem.at[r]) for r in range(regions)
    ]
    small = [
        pltpu.make_async_copy(src, dst, small_sem.at[n])
        for n, (src, dst) in enumerate(
            [
                (count_hbm, count_ref),
                (radius_hbm, radius_ref),
                (innov_hbm.at[0], innov_ref),
                (weight_hbm.at[0], weight_ref),
                (column_hbm.at[0], column_ref),
                (states_hbm, anomaly),
            ]
        )
    ]
    for load in small[:-1] + loads + small[-1:]:
        load.start()

    barrier = pltpu.get_barrier_semaphore()
    peers = [lax.rem(tm + d, n_tm) for d in range(1, n_tm)]
    greeted = [(p, sp) for p in peers]
    greeted += [(t, s) for s in (before, after) for t in range(n_tm)]
    for t, s in greeted:
        pl.semaphore_signal(barrier, inc=1, device_id={"tm": t, "space": s}, device_id_type=MESH)

    for load in small[:-1]:
        load.wait()

    shape = (regions, capacity)
    which = iota2(shape, 0)
    count = jnp.zeros(shape, jnp.int32)
    radius = jnp.zeros(shape, jnp.int32)
    for r in range(regions):
        count = jnp.where(which == r, count_ref[0, r], count)
        radius = jnp.where(which == r, radius_ref[r], radius)
    present = (iota2(shape, 1) < count).astype(F32)
    base = weight_ref[...] * present
    inverse_radius = 1.0 / radius.astype(F32)
    position = column_ref[...].astype(F32) + 0.5 - 0.5 * HC
    weights, pulls = [], []
    for offset in range(-HALO, HALO + 1):
        ratio = jnp.minimum(jnp.abs(position - offset * HC) * inverse_radius, 1.0)
        weight = base * jnp.square(1.0 - ratio * ratio)
        weights.append(weight)
        pulls.append(weight * innov_ref[...])

    first_row = iota2((EXTRA, capacity), 0) == 0

    def gram_of(target):
        total = None
        for r in range(max(0, target - 2 * HALO), min(regions, target + 1)):
            k = target - r
            weight = jnp.broadcast_to(weights[k][r : r + 1], (16, capacity)).astype(BF16)
            pull = jnp.where(first_row, pulls[k][r : r + 1], 0.0).astype(BF16)
            scaled = obs_t[r].reshape(members // 16, 16, capacity) * weight[None]
            left = jnp.concatenate([scaled.reshape(members, capacity), pull], axis=0)
            part = jnp.dot(left, obs_v[r], preferred_element_type=F32)
            total = part if total is None else total + part
        top, extra = pack(total[:members], total[members : members + 1])
        mine[target, :half] = top.astype(BF16)
        mine[target, half:] = extra.astype(BF16)

    height = mine.shape[1]
    whole = pl.ds(0, height)
    cut = height // (2 * EXTRA) * EXTRA
    chunks = [pl.ds(0, cut), pl.ds(cut, height - cut)]

    def exchange(kind, sem, block_of, rows):
        copies = []
        for d, peer in enumerate(peers):
            copies.append(
                pltpu.make_async_remote_copy(
                    src_ref=mine.at[block_of(peer), rows],
                    dst_ref=recv.at[kind, tm, rows],
                    send_sem=rs_send.at[sem, d],
                    recv_sem=rs_recv.at[sem, tm],
                    device_id={"tm": peer, "space": sp},
                    device_id_type=MESH,
                )
            )
        return copies

    def collect(kind, sem, block, rows):
        total = mine[block, rows].astype(F32)
        for peer in peers:
            landed = recv.at[kind, peer, rows]
            pltpu.make_async_copy(landed, landed, rs_recv.at[sem, peer]).wait()
            total = total + recv[kind, peer, rows].astype(F32)
        return total

    ready = 0
    for target in [*range(HALO), *range(targets - HALO, targets)]:
        while ready < min(regions, target + 1):
            loads[ready].wait()
            obs_t[ready] = obs_v[ready].T
            ready += 1
        gram_of(target)
    pl.semaphore_wait(barrier, len(greeted))
    edge_block = lambda p: lax.rem(p + regions + HALO, targets)
    inner_block = lambda p: p + HALO
    edge_copies = []
    for c, part in enumerate(chunks):
        edge_copies += exchange(0, c + 1, edge_block, part)
    for copy in edge_copies:
        copy.start()
    inner = list(range(HALO, targets - HALO))
    for target in inner:
        gram_of(target)
    inner_copies = exchange(1, 0, inner_block, whole)
    for copy in inner_copies:
        copy.start()

    small[-1].wait()
    lags, _, rows, _ = anomaly.shape

    def centre_on_mean(n, carry):
        lag, r = n // regions, lax.rem(n, regions)
        x = anomaly[lag, r].astype(F32)
        mean = jnp.sum(x, axis=1, keepdims=True) * (1.0 / members)
        means[lag, r] = mean
        anomaly[lag, r] = (x - mean).astype(BF16)
        return carry

    lax.fori_loop(0, lags * regions, centre_on_mean, 0)

    halo_copies = []
    for c, part in enumerate(chunks):
        halo_out[part] = collect(0, c + 1, edge_block(tm), part).astype(BF16)
        halo_copies.append(
            pltpu.make_async_remote_copy(
                src_ref=halo_out.at[part],
                dst_ref=halo_in.at[part],
                send_sem=halo_send.at[c],
                recv_sem=halo_recv.at[c],
                device_id={"tm": tm, "space": jnp.where(tm < HALO, after, before)},
                device_id_type=MESH,
            )
        )
        halo_copies[c].start()
    total = collect(1, 0, inner_block(tm), whole)
    for copy in halo_copies:
        copy.wait()
    gram, vec = unpack(total + halo_in[...].astype(F32))
    spread, wbar = transform_parts(gram, vec)
    top, extra = pack(spread, wbar)
    t_out[:half] = top.astype(BF16)
    t_out[half:] = extra.astype(BF16)

    def send_transform(t, s, slot, sem):
        return pltpu.make_async_remote_copy(
            src_ref=t_out,
            dst_ref=t_in.at[slot],
            send_sem=sem,
            recv_sem=t_recv.at[slot],
            device_id={"tm": t, "space": s},
            device_id_type=MESH,
        )

    low = [send_transform(t, before, regions + 1, b_send.at[t]) for t in range(n_tm)]
    high = [send_transform(t, after, 0, b_send.at[t]) for t in range(n_tm)]

    @pl.when(tm == 0)
    def _():
        for copy in reversed(low):
            copy.start()

    @pl.when(tm == n_tm - 1)
    def _():
        for copy in high:
            copy.start()

    t_copies = [send_transform(p, sp, tm + 1, t_send.at[d]) for d, p in enumerate(peers)]
    for copy in t_copies:
        copy.start()

    def place(slot, block):
        matrix, row = unpack(block.astype(F32))
        tmat[slot] = (matrix + row).astype(BF16)

    def arrive(slot):
        pltpu.make_async_copy(t_in.at[slot], t_in.at[slot], t_recv.at[slot]).wait()
        place(slot, t_in[slot])

    mid = rows // 2

    def update(r, side):
        part = slice(side * mid, (side + 1) * mid)
        column = (iota2((mid, 1), 0) + side * mid) // (rows // HC)
        blend = jnp.abs((column.astype(F32) + 0.5) / HC - 0.5)
        for lag in range(lags):
            block = anomaly[lag, r, part]

            def apply(slot):
                return lax.dot_general(
                    block, tmat[slot], (((1,), (1,)), ((), ())), preferred_element_type=F32
                )

            centre, beside = apply(r + 1), apply(r + 2 * side)
            mean = means[lag, r, part]
            out_ref[lag, r, part] = (mean + centre + blend * (beside - centre)).astype(BF16)

    place(tm + 1, t_out[...])
    for d in range(1, n_tm):
        arrive(lax.rem(tm + d, n_tm) + 1)
    for r in range(regions):
        for side in range(2):
            if (r, side) not in ((0, 0), (regions - 1, 1)):
                update(r, side)
    arrive(0)
    update(0, 0)
    arrive(regions + 1)
    update(regions - 1, 1)

    for copy in edge_copies + inner_copies + t_copies:
        copy.wait_send()

    @pl.when(tm == 0)
    def _():
        for copy in low:
            copy.wait_send()

    @pl.when(tm == n_tm - 1)
    def _():
        for copy in high:
            copy.wait_send()


def shards(n_tm, n_space, obs, innovation, error_weight, obs_column, obs_count, radius, states):
    _, regions, capacity, members = obs.shape
    assert regions == n_tm and obs.shape[0] == 1
    rows = members // 2 + EXTRA
    lags, columns, levels, _ = states.shape
    shaped = states.reshape(lags, regions, columns // regions * levels, members)
    hbm = pl.BlockSpec(memory_space=pltpu.HBM)
    dma = pltpu.SemaphoreType.DMA
    result = pl.pallas_call(
        functools.partial(assimilate, n_tm, n_space),
        out_shape=pltpu.VMEM(shaped.shape, BF16),
        in_specs=[hbm] * 7,
        out_specs=pl.BlockSpec(memory_space=pltpu.VMEM),
        scratch_shapes=[
            pltpu.SMEM(obs_count.shape, jnp.int32),
            pltpu.SMEM(radius.shape, jnp.int32),
            pltpu.VMEM((regions, capacity), F32),
            pltpu.VMEM((regions, capacity), F32),
            pltpu.VMEM((regions, capacity), jnp.int32),
            pltpu.VMEM(shaped.shape, BF16),
            pltpu.VMEM(shaped.shape[:-1] + (1,), F32),
            pltpu.VMEM((regions + 2, members, members), BF16),
            pltpu.VMEM((regions, capacity, members), BF16),
            pltpu.VMEM((regions, members, capacity), BF16),
            pltpu.VMEM((regions + 2 * HALO, rows, members), BF16),
            pltpu.VMEM((2, n_tm, rows, members), BF16),
            pltpu.VMEM((rows, members), BF16),
            pltpu.VMEM((rows, members), BF16),
            pltpu.VMEM((rows, members), BF16),
            pltpu.VMEM((regions + 2, rows, members), BF16),
            dma((regions,)),
            dma((6,)),
            dma((3, n_tm - 1)),
            dma((3, n_tm)),
            dma((2,)),
            dma((2,)),
            dma((n_tm - 1,)),
            dma((n_tm,)),
            dma((regions + 2,)),
        ],
        compiler_params=pltpu.CompilerParams(
            collective_id=0, has_side_effects=True, vmem_limit_bytes=67043328 - 2228224
        ),
        name="assimilate",
    )(obs_count, radius, obs, innovation, error_weight, obs_column, shaped)
    return result.reshape(states.shape)


def solution(mesh):
    return jax.shard_map(
        functools.partial(shards, mesh.shape["tm"], mesh.shape["space"]),
        mesh=mesh,
        in_specs=(
            P("tm", "space", None, None),
            P("tm", "space", None),
            P("tm", "space", None),
            P("tm", "space", None),
            P("tm", "space"),
            P("space"),
            P("tm", "space", None, None),
        ),
        out_specs=P("tm", "space", None, None),
        check_vma=False,
    )
```
